32 devices in a mesh: lon: 8 (over z, x), lat: 4 (over y, core).
Axes of the slice: x: 2, y: 2, z: 4, core: 2. Of those that a mesh axis runs over, the one named last changes fastest.
Arguments:
- state: float32 [8, 64, 16, 1024], P(None, None, 'lat', 'lon'), may hold values from -6 to 6
- winds: float32 [2, 64, 16, 1024], P(None, None, 'lat', 'lon'), may hold values from -0.3 to 0.3
- diffusivity: float32 [16, 1024], P('lat', 'lon'), may hold values from 0.05 to 0.2
- sounding_cell: int32 [2, 4096], P(None, ('lon', 'lat')), may hold values from 0 to 511
- sounding_owner: int32 [2, 4096, 1], P(None, ('lon', 'lat')), may hold values from 0 to 31; in each aligned block of 128 rows (0 to 127, 128 to 255, ..., all dimensions but the last counted through in order) at most 6 rows name the same one
- step_counts: int32 [2], replicated, may hold values from 1 to 4
- channel_list: int32 [512], replicated, may hold values from 0 to 615
- absorb_table: float32 [512, 616], replicated, may hold values from -0.25 to 0.25
- emit_table: float32 [512, 616], replicated, may hold values from -0.25 to 0.25
- obs_weight: float32 [616], replicated, may hold values from 0.5 to 4
- observed: float32 [2, 32, 32, 6, 512], P(None, ('lon', 'lat')), may hold values from -6 to 6
Outputs:
- gradient: float32 [8, 64, 16, 1024], P(None, None, 'lat', 'lon')
The draws below stay inside these ranges and needn't reach their ends.
Inputs may be any that keep to these rules, and one draw needn't show every extreme that they name: `sounding_owner`: in one slot, at most 6 soundings of one tile's list name the same owner. `sounding_cell`: columns are numbered row by row within the tile. `channel_list`: entries may repeat.
All inputs are finite; a program needn't handle non-finite values.
Results may differ from the reference program's by a relative error of at most 0.00022.
Values sent between devices are 32-bit elements; how exact they have to be, the bound alone decides.
A program may use at most 128 MiB of HBM per device.

```python
import math
from functools import partial
import jax
import jax.numpy as jnp
import numpy as np
from jax import lax

VARS = 8
LEV = 64
CHAN = 616
USED = 512
CLAT = 4
CLON = 128
SND = 128
MAXSTEP = 4
SLOTS = 2
PROF = 512
NLAT = 16
NLON = 1024
SOUNDINGS = 4096
CAP = 6
N_LAT = 4
DEVICES = 32


def plant(drawn, rng, smallest, top_value):
    longest = drawn.shape.index(max(drawn.shape))
    spots = []
    for shift in (0, 1):
        where = [jax.random.randint(jax.random.fold_in(rng, axis), (), 0, length) for axis, length in enumerate(drawn.shape)]
        where[longest] = (where[longest] + shift) % drawn.shape[longest]
        spots.append(tuple(where))
    return drawn.at[spots[0]].set(smallest).at[spots[1]].set(top_value)


def level_of(rng, dims, cuts, least, largest):
    def one(position, blocks):
        steps = jax.random.uniform(jax.random.fold_in(jax.random.fold_in(rng, 6), position), (blocks,), jnp.float32, least / len(cuts), largest / len(cuts))
        return jnp.repeat(jnp.exp(steps), dims[position] // blocks).reshape((-1,) + (1,) * (len(dims) - position - 1))

    level = one(*cuts[0])
    for cut in cuts[1:]:
        level = level * one(*cut)
    return level


def assign_block(rng, own, number, rows, count, top, most, slope):
    order = jax.random.permutation(rng, count)
    packed, ordinary = load_shares(count, rows * top, most, slope, True), load_shares(count, rows * top, most, slope, False)
    places = jnp.arange(count)

    def named(sizes, offset_by):
        used = int((sizes > 0).sum())
        fixed = max(1, used // 4)
        shifted = fixed + (places - fixed + offset_by * (used - fixed)) % max(1, count - fixed)
        return jnp.zeros((count,), jnp.int32).at[order[jnp.where(places < fixed, places, shifted)]].set(jnp.asarray(sizes, jnp.int32))

    sizes = jnp.where(number % 4 == 0, named(packed, number // 4), named(ordinary, number - number // 4 - 1))
    mixed = jax.random.permutation(jax.random.fold_in(own, 3), count)
    source_of, taker = mixed[0:count // 2 * 2:2], mixed[1:count // 2 * 2:2]
    margin = jnp.minimum(sizes[source_of] - 1, most - sizes[taker]) // 2
    margin = jnp.where((source_of == order[0]) | (taker == order[0]) | (sizes[taker] == 0), 0, jnp.maximum(margin, 0))
    shifted = jax.random.randint(jax.random.fold_in(own, 4), (count // 2,), 0, 1 << 20) % (margin + 1)
    sizes = sizes.at[source_of].add(-shifted).at[taker].add(shifted)
    labels = jnp.searchsorted(jnp.cumsum(sizes), jnp.arange(rows * top), side="right").astype(jnp.int32)
    grid = labels.reshape(top, rows).T
    grid = grid[jax.random.permutation(jax.random.fold_in(own, 1), rows)]
    offset_by = jax.random.randint(jax.random.fold_in(own, 2), (rows, 1), 0, top)
    return jnp.take_along_axis(grid, (jnp.arange(top)[None, :] + offset_by) % top, axis=1)


def load_shares(count, total, most, skew, full):
    loads = [(1 << 20) // math.isqrt(grade ** skew) + 1 for grade in range(1, count + 1)]
    largest = most if full else min(most, max(-(-total // count), total * loads[0] // sum(loads)))
    least = 1 if total - largest >= count - 1 else 0
    counts, surplus = [largest] + [least] * (count - 1), total - largest - least * (count - 1)
    while surplus > 0:
        movable = [i for i in range(1, count) if counts[i] < largest] or [i for i in range(1, count) if counts[i] < most]
        mass, budget = sum([loads[i] for i in movable]), surplus
        for i in movable:
            extra = min(most - counts[i], max(1, budget * loads[i] // mass), surplus)
            counts[i] = counts[i] + extra
            surplus = surplus - extra
    return np.array(counts)


def centred(own_key, extent, deviation, reach, split=(), kind=jnp.bfloat16):
    values = jax.random.normal(own_key, extent, jnp.float32) * deviation
    if len(split) > 0:
        values = level_of(own_key, extent, split, -0.22, 0.18) * values
    return jnp.clip(values, min=-reach, max=reach).astype(kind)


def setup_inputs(seed: int = 0) -> dict:
    key_list = jax.random.split(jax.random.key(seed), 12)
    state = centred(key_list[0], (VARS, LEV, NLAT, NLON), 1.0, 6.0, ((2, 4), (3, 8)), jnp.float32)
    winds = jnp.clip(jax.random.uniform(key_list[1], (2, LEV, NLAT, NLON), jnp.float32, -0.3, 0.3) * level_of(key_list[1], (2, LEV, NLAT, NLON), ((2, 4), (3, 8)), -0.4, 0.0), -0.3, 0.3)
    diffusivity = jnp.clip(0.05 + 0.15 * jax.random.uniform(key_list[2], (NLAT, NLON), jnp.float32) ** level_of(key_list[2], (NLAT, NLON), ((0, 4), (1, 8)), -0.2, 0.2), 0.05, 0.2)
    sounding_cell = plant(jax.random.randint(key_list[3], (SLOTS, SOUNDINGS), 0, CLAT * CLON), jax.random.fold_in(key_list[3], 1), 0, (CLAT * CLON) - 1).astype(jnp.int32)
    sounding_owner_keys = jax.random.split(jax.random.fold_in(key_list[4], 1), SLOTS * SOUNDINGS // SND)
    sounding_owner_turns = jax.random.permutation(jax.random.fold_in(key_list[4], 3), SLOTS * SOUNDINGS // SND)
    sounding_owner = jax.vmap(lambda own, number: assign_block(jax.random.fold_in(key_list[4], 2), own, number, SND, DEVICES, 1, CAP, 2))(sounding_owner_keys, sounding_owner_turns).reshape((SLOTS, SOUNDINGS, 1))
    step_counts = jax.random.randint(key_list[5], (SLOTS,), 1, MAXSTEP + 1).astype(jnp.int32)
    channel_list = plant(jax.random.randint(key_list[6], (USED,), 0, CHAN), jax.random.fold_in(key_list[6], 1), 0, CHAN - 1).astype(jnp.int32)
    absorb_table = centred(key_list[7], (PROF, CHAN), PROF ** -0.5, 0.25, (), jnp.float32)
    emit_table = centred(key_list[8], (PROF, CHAN), PROF ** -0.5, 0.25, (), jnp.float32)
    obs_weight = jnp.clip(jnp.exp(jax.random.uniform(key_list[9], (CHAN,), jnp.float32, math.log(0.5), math.log(4.0))), 0.5, 4.0)
    observed = centred(key_list[10], (SLOTS, DEVICES, DEVICES, CAP, USED), 1.0, 6.0, ((1, 32),), jnp.float32)
    return {"state": state, "winds": winds, "diffusivity": diffusivity, "sounding_cell": sounding_cell, "sounding_owner": sounding_owner, "step_counts": step_counts, "channel_list": channel_list, "absorb_table": absorb_table, "emit_table": emit_table, "obs_weight": obs_weight, "observed": observed}


HIGHEST_MODE = lax.Precision.HIGHEST

def pad_field(values):
    wrapped = jnp.concatenate([values[..., -1:], values, values[..., :1]], axis=-1)
    widths = [(0, 0)] * (values.ndim - 2) + [(1, 1), (0, 0)]
    return jnp.pad(wrapped, widths)

def make_coef(winds, diffusivity):
    return jnp.stack([winds[0] * 0.5 + diffusivity, winds[0] * 0.5 - diffusivity, winds[1] * 0.5 + diffusivity, winds[1] * 0.5 - diffusivity])

def advance(padded, coef_pad):
    centre = padded[:, :, 1:-1, 1:-1]
    lon_band = padded[:, :, 1:-1, :]
    flux_lon = coef_pad[0][:, 1:-1, :-1] * lon_band[..., :-1] + coef_pad[1][:, 1:-1, :-1] * lon_band[..., 1:]
    lat_band = padded[:, :, :, 1:-1]
    flux_lat = coef_pad[2][:, :-1, 1:-1] * lat_band[:, :, :-1, :] + coef_pad[3][:, :-1, 1:-1] * lat_band[:, :, 1:, :]
    return centre - (flux_lon[..., 1:] - flux_lon[..., :-1]) - (flux_lat[:, :, 1:, :] - flux_lat[:, :, :-1, :])

def retreat(padded, coef_pad):
    centre = padded[:, :, 1:-1, 1:-1]
    lon_band = padded[:, :, 1:-1, :]
    step_lon = lon_band[..., 1:] - lon_band[..., :-1]
    result = centre + coef_pad[0][:, 1:-1, 1:-1] * step_lon[..., 1:] + coef_pad[1][:, 1:-1, :-2] * step_lon[..., :-1]
    lat_band = padded[:, :, :, 1:-1]
    step_lat = lat_band[:, :, 1:, :] - lat_band[:, :, :-1, :]
    result = result + coef_pad[2][:, 1:-1, 1:-1] * step_lat[:, :, 1:, :] + coef_pad[3][:, :-2, 1:-1] * step_lat[:, :, :-1, :]
    return result

def select_channels(channel_list, absorb_table, emit_table, obs_weight):
    picker = (jnp.arange(obs_weight.shape[0], dtype=jnp.int32)[:, None] == channel_list[None, :]).astype(jnp.float32)
    absorb = jnp.dot(absorb_table, picker, precision=HIGHEST_MODE, preferred_element_type=jnp.float32)
    emission = jnp.dot(emit_table, picker, precision=HIGHEST_MODE, preferred_element_type=jnp.float32)
    weight = jnp.dot(obs_weight[None, :], picker, precision=HIGHEST_MODE, preferred_element_type=jnp.float32)[0]
    return (absorb, emission, weight)

def radiance(profiles, absorb, emission):
    optical = jnp.dot(profiles, absorb, precision=HIGHEST_MODE, preferred_element_type=jnp.float32)
    bright = jnp.dot(profiles, emission, precision=HIGHEST_MODE, preferred_element_type=jnp.float32)
    return jnp.exp(-jax.nn.softplus(optical)) * bright

def slot_gradient(state_now, slot_index, sounding_cell, sounding_owner, observed, absorb, emission, weight):
    sounding_cells = sounding_cell[slot_index].reshape(DEVICES, SND)
    owners = sounding_owner[slot_index, :, 0].reshape(DEVICES, SND)
    owner_hit = (owners[:, :, None] == jnp.arange(DEVICES, dtype=jnp.int32)[None, None, :]).astype(jnp.int32)
    owner_rank = lax.optimization_barrier(jnp.sum(jnp.cumsum(owner_hit, axis=1) * owner_hit, axis=2)) - 1
    home_index = jnp.broadcast_to(jnp.arange(DEVICES, dtype=jnp.int32)[:, None], (DEVICES, SND))
    wanted = observed[slot_index, owners, home_index, owner_rank].reshape(DEVICES * SND, USED)
    lat_rows = (home_index % N_LAT * CLAT + sounding_cells // CLON).reshape(-1).astype(jnp.int32)
    lon_cols = (home_index // N_LAT * CLON + sounding_cells % CLON).reshape(-1).astype(jnp.int32)
    profiles = state_now[:, :, lat_rows, lon_cols].reshape(PROF, DEVICES * SND).T
    evolved, pullback = jax.vjp(partial(radiance, absorb=absorb, emission=emission), profiles)
    departure = weight[None, :] * (evolved - wanted)
    adjoint_cols = pullback(departure)[0]
    placed = adjoint_cols.T.reshape(VARS, LEV, DEVICES * SND)
    return jnp.zeros_like(state_now).at[:, :, lat_rows, lon_cols].add(placed)

def reference(state, winds, diffusivity, sounding_cell, sounding_owner, step_counts, channel_list, absorb_table, emit_table, obs_weight, observed):
    coef_pad = pad_field(make_coef(winds, diffusivity))
    absorb, emission, weight = select_channels(channel_list, absorb_table, emit_table, obs_weight)
    state_now = state
    slot_fields = []
    for slot_index in range(SLOTS):
        for step_index in range(MAXSTEP):
            state_now = jnp.where(step_index < step_counts[slot_index], advance(pad_field(state_now), coef_pad), state_now)
        slot_fields.append(state_now)
    gradients = [slot_gradient(slot_fields[slot_index], slot_index, sounding_cell, sounding_owner, observed, absorb, emission, weight) for slot_index in range(SLOTS)]
    adjoint = jnp.zeros_like(state)
    for slot_index in reversed(range(SLOTS)):
        adjoint = adjoint + gradients[slot_index]
        for step_index in range(MAXSTEP):
            adjoint = jnp.where(step_index < step_counts[slot_index], retreat(pad_field(adjoint), coef_pad), adjoint)
    return adjoint
```

```python
from functools import partial

import jax
import jax.numpy as jnp
from jax import lax
from jax.experimental import pallas as pl
from jax.experimental.pallas import tpu as pltpu
from jax.sharding import PartitionSpec as P

MAXSTEP = 4
LANES = 128
PAD = 8
MESH_ID = pl.DeviceIdType.MESH


def march_kernel(steps, lat_count, lon_count, x_ref, c_ref, o_ref, X, HL, ST, send_sem, recv_sem):
    groups, rows, width, _ = x_ref.shape
    lat = lax.axis_index("lat")
    lon = lax.axis_index("lon")
    east = lax.rem(lon + 1, lon_count)
    west = lax.rem(lon + lon_count - 1, lon_count)
    has_up = lat > 0
    has_down = lat < lat_count - 1
    inner = pl.ds(PAD, width)

    barrier = pltpu.get_barrier_semaphore()

    def greet(lat_to, lon_to):
        pl.semaphore_signal(barrier, inc=1, device_id={"lon": lon_to, "lat": lat_to}, device_id_type=MESH_ID)

    greet(lat, east)
    greet(lat, west)

    @pl.when(has_up)
    def _():
        greet(lat - 1, lon)

    @pl.when(has_down)
    def _():
        greet(lat + 1, lon)

    def to_up(p, g):
        return pltpu.make_async_remote_copy(
            X.at[p, g, 1, inner], X.at[p, g, rows + 1, inner],
            send_sem.at[p, g, 0], recv_sem.at[p, g, 0],
            device_id={"lon": lon, "lat": lat - 1}, device_id_type=MESH_ID)

    def to_down(p, g):
        return pltpu.make_async_remote_copy(
            X.at[p, g, rows, inner], X.at[p, g, 0, inner],
            send_sem.at[p, g, 1], recv_sem.at[p, g, 1],
            device_id={"lon": lon, "lat": lat + 1}, device_id_type=MESH_ID)

    def to_east(p, g):
        return pltpu.make_async_remote_copy(
            ST.at[p, g, 0], HL.at[p, g, 0],
            send_sem.at[p, g, 2], recv_sem.at[p, g, 2],
            device_id={"lon": east, "lat": lat}, device_id_type=MESH_ID)

    def to_west(p, g):
        return pltpu.make_async_remote_copy(
            ST.at[p, g, 1], HL.at[p, g, 1],
            send_sem.at[p, g, 3], recv_sem.at[p, g, 3],
            device_id={"lon": west, "lat": lat}, device_id_type=MESH_ID)

    def send(p, g):
        for r in range(rows):
            ST[p, g, 0, pl.ds(r, 1), :] = X[p, g, r + 1, pl.ds(PAD + width - 1, 1), :]
            ST[p, g, 1, pl.ds(r, 1), :] = X[p, g, r + 1, pl.ds(PAD, 1), :]

        @pl.when(has_up)
        def _():
            to_up(p, g).start()

        @pl.when(has_down)
        def _():
            to_down(p, g).start()

        to_east(p, g).start()
        to_west(p, g).start()

    def wait_send(p, g):
        @pl.when(has_up)
        def _():
            to_up(p, g).wait_send()

        @pl.when(has_down)
        def _():
            to_down(p, g).wait_send()

        to_east(p, g).wait_send()
        to_west(p, g).wait_send()

    def wait_recv(p, g):
        @pl.when(has_down)
        def _():
            to_up(p, g).wait_recv()

        @pl.when(has_up)
        def _():
            to_down(p, g).wait_recv()

        to_east(p, g).wait_recv()
        to_west(p, g).wait_recv()

    edge = jnp.zeros((width, LANES), jnp.float32)

    @pl.loop(0, groups)
    def _(g):
        for r in range(rows):
            X[0, g, r + 1, inner, :] = x_ref[g, r]
        for p in range(2):
            ST[p, g] = jnp.zeros(ST.shape[2:], jnp.float32)

            @pl.when(jnp.logical_not(has_up))
            def _():
                X[p, g, 0, inner, :] = edge

            @pl.when(jnp.logical_not(has_down))
            def _():
                X[p, g, rows + 1, inner, :] = edge

    pl.semaphore_wait(barrier, 2 + has_up.astype(jnp.int32) + has_down.astype(jnp.int32))

    @pl.loop(0, groups)
    def _(g):
        send(0, g)

    @pl.loop(0, steps * groups)
    def _(it):
        s = it // groups
        g = it % groups
        p = s % 2
        q = 1 - p
        wait_recv(p, g)

        @pl.when(s > 0)
        def _():
            wait_send(q, g)

        for r in range(rows):
            X[p, g, r + 1, pl.ds(PAD - 1, 1), :] = HL[p, g, 0, pl.ds(r, 1), :]
            X[p, g, r + 1, pl.ds(PAD + width, 1), :] = HL[p, g, 1, pl.ds(r, 1), :]
        for r in range(rows):
            for b in range(0, width, 64):
                at = pl.ds(PAD + b, 64)
                cat = pl.ds(b, 64)
                new = c_ref[0, r, cat, :] * X[p, g, r + 1, at, :]
                new = new + c_ref[3, r, cat, :] * X[p, g, r + 2, at, :]
                new = new + c_ref[4, r, cat, :] * X[p, g, r, at, :]
                new = new + c_ref[1, r, cat, :] * X[p, g, r + 1, pl.ds(PAD + b + 1, 64), :]
                new = new + c_ref[2, r, cat, :] * X[p, g, r + 1, pl.ds(PAD + b - 1, 64), :]
                X[q, g, r + 1, at, :] = new

        @pl.when(s < steps - 1)
        def _():
            send(q, g)

    @pl.loop(0, groups)
    def _(g):
        wait_send((steps - 1) % 2, g)
        for r in range(rows):
            o_ref[g, r] = X[steps % 2, g, r + 1, inner, :]


def march_call(steps, lat_count, lon_count, values, coef):
    groups, rows, width, lanes = values.shape
    edge_rows = -(-rows // 8) * 8
    vmem = pl.BlockSpec(memory_space=pltpu.VMEM)
    return pl.pallas_call(
        partial(march_kernel, steps, lat_count, lon_count),
        out_shape=jax.ShapeDtypeStruct(values.shape, jnp.float32),
        in_specs=[vmem, vmem],
        out_specs=vmem,
        scratch_shapes=[
            pltpu.VMEM((2, groups, rows + 2, width + 2 * PAD, lanes), jnp.float32),
            pltpu.VMEM((2, groups, 2, edge_rows, lanes), jnp.float32),
            pltpu.VMEM((2, groups, 2, edge_rows, lanes), jnp.float32),
            pltpu.SemaphoreType.DMA((2, groups, 4)),
            pltpu.SemaphoreType.DMA((2, groups, 4)),
        ],
        compiler_params=pltpu.CompilerParams(
            collective_id=steps, has_side_effects=True, vmem_limit_bytes=16 << 20
        ),
        cost_estimate=pl.CostEstimate(
            flops=9 * steps * values.size, bytes_accessed=8 * values.size * steps, transcendentals=0
        ),
        name="march",
    )(values, coef)


def march(values, count, coef, lat_count, lon_count):
    branches = [partial(march_call, n, lat_count, lon_count) for n in range(1, MAXSTEP + 1)]
    return lax.switch(count - 1, branches, values, coef)


def split2(v):
    high = v.astype(jnp.bfloat16)
    return high, (v - high.astype(jnp.float32)).astype(jnp.bfloat16)


def split3(v):
    high = v.astype(jnp.bfloat16)
    rest = v - high.astype(jnp.float32)
    mid = rest.astype(jnp.bfloat16)
    return high, mid, (rest - mid.astype(jnp.float32)).astype(jnp.bfloat16)


def dot(a, b, dims=((1,), (0,))):
    return lax.dot_general(a, b, (dims, ((), ())), preferred_element_type=jnp.float32)


def pick(chosen, v, dims=((1,), (0,))):
    high, mid, low = split3(v)
    return dot(chosen, high, dims) + dot(chosen, mid, dims) + dot(chosen, low, dims)


def product(a, b, dims=((1,), (0,))):
    return dot(a[0], b[0], dims) + dot(a[0], b[1], dims) + dot(a[1], b[0], dims)


def one_hot(column, size):
    return (column == lax.broadcasted_iota(jnp.int32, (column.shape[0], size), 1)).astype(
        jnp.float32).astype(jnp.bfloat16)


def obs_kernel(capacity, x0_ref, x1_ref, cell_ref, own_col_ref, own_row_ref, got_ref, chan_ref,
               absorb_ref, emit_ref, weight_ref, g0_ref, g1_ref):
    groups, cells, lanes = x0_ref.shape
    soundings = cell_ref.shape[1]
    channels = weight_ref.shape[1]
    fields = (x0_ref, x1_ref)
    outs = (g0_ref, g1_ref)
    picker = one_hot(chan_ref[...], channels)
    count = jnp.sum(picker.astype(jnp.float32), axis=0, keepdims=True)
    absorb = split2(absorb_ref[...])
    emit = split2(emit_ref[...])
    weight = weight_ref[...]
    for k in range(2):
        placed = one_hot(cell_ref[k], cells)
        owner = own_col_ref[k]
        earlier = lax.broadcasted_iota(jnp.int32, (soundings, soundings), 1) < lax.broadcasted_iota(
            jnp.int32, (soundings, soundings), 0)
        same = jnp.logical_and(owner == own_row_ref[k], earlier)
        rank = jnp.sum(same.astype(jnp.float32), axis=1, keepdims=True).astype(jnp.int32)
        source = one_hot(owner * capacity + rank, got_ref.shape[1])
        wanted = pick(picker, pick(source, got_ref[k]), ((0,), (1,)))
        wanted = wanted.T
        profile = jnp.concatenate([pick(placed, fields[k][g]) for g in range(groups)], axis=1)
        profile = split2(profile)
        optical = product(profile, absorb)
        bright = product(profile, emit)
        small = jnp.exp(-jnp.abs(optical))
        inv = 1.0 / (1.0 + small)
        passed = jnp.where(optical > 0, small, 1.0) * inv
        slope = jnp.where(optical > 0, 1.0, small) * inv
        y = passed * bright
        departure = weight * (count * y - wanted)
        d_bright = split2(departure * passed)
        d_optical = split2(-(departure * y) * slope)
        back = product(d_optical, absorb, ((1,), (1,))) + product(d_bright, emit, ((1,), (1,)))
        for g in range(groups):
            outs[k][g] = pick(placed, back[:, g * lanes:(g + 1) * lanes], ((0,), (0,)))


def observe(x0, x1, sounding_cell, owners, fetched, channel_list, absorb, emit, weight, capacity):
    groups, rows, width, lanes = x0.shape
    flat = (groups, rows * width, lanes)
    vmem = pl.BlockSpec(memory_space=pltpu.VMEM)
    g0, g1 = pl.pallas_call(
        partial(obs_kernel, capacity),
        out_shape=[jax.ShapeDtypeStruct(flat, jnp.float32)] * 2,
        in_specs=[vmem] * 10,
        out_specs=[vmem] * 2,
        compiler_params=pltpu.CompilerParams(vmem_limit_bytes=56 << 20),
        cost_estimate=pl.CostEstimate(flops=6 << 30, bytes_accessed=8 << 20, transcendentals=0),
        name="observe",
    )(x0.reshape(flat), x1.reshape(flat), sounding_cell[:, :, None], owners[:, :, None],
      owners[:, None, :], fetched, channel_list[:, None], absorb, emit, weight[None, :])
    return g0.reshape(x0.shape), g1.reshape(x0.shape)


def coefficients(winds, diffusivity, lat_count, lon_count):
    levels = winds.shape[1]
    w = jnp.transpose(winds, (0, 2, 3, 1))
    w = jnp.concatenate([w] * (LANES // levels), axis=-1) * 0.5
    d = diffusivity[:, :, None]
    lon_pair = jnp.stack([w[0] + d, w[0] - d])
    lat_pair = jnp.stack([w[1] + d, w[1] - d])
    west_edge = lax.ppermute(lon_pair[:, :, -1:], "lon", [(i, (i + 1) % lon_count) for i in range(lon_count)])
    up_edge = lax.ppermute(lat_pair[:, -1:], "lat", [(i, i + 1) for i in range(lat_count - 1)])
    lon_west = jnp.concatenate([west_edge, lon_pair[:, :, :-1]], axis=2)
    lat_up = jnp.concatenate([up_edge, lat_pair[:, :-1]], axis=1)
    a, b = lon_pair[0], lon_pair[1]
    aw, bw = lon_west[0], lon_west[1]
    al, bl = lat_pair[0], lat_pair[1]
    au, bu = lat_up[0], lat_up[1]
    centre = 1.0 - a + bw - al + bu
    forward = jnp.stack([centre, -b, aw, -bl, au])
    backward = jnp.stack([centre, a, -bw, al, -bu])
    return forward, backward


def per_device(lat_count, lon_count, state, winds, diffusivity, sounding_cell, sounding_owner,
               step_counts, channel_list, absorb_table, emit_table, obs_weight, observed):
    variables, levels, rows, width = state.shape
    groups = variables * levels // LANES
    slots, _, devices, capacity, used = observed.shape
    fetched = lax.all_to_all(observed[:, 0], ("lon", "lat"), split_axis=1, concat_axis=1, tiled=True)
    fetched = fetched.reshape(slots, devices * capacity, used)
    forward, backward = coefficients(winds, diffusivity, lat_count, lon_count)
    x = jnp.transpose(state.reshape(groups, LANES, rows * width), (0, 2, 1)).reshape(
        groups, rows, width, LANES)
    x0 = march(x, step_counts[0], forward, lat_count, lon_count)
    x1 = march(x0, step_counts[1], forward, lat_count, lon_count)
    g0, g1 = observe(x0, x1, sounding_cell, sounding_owner[:, :, 0], fetched, channel_list,
                     absorb_table, emit_table, obs_weight, capacity)
    back = march(g1, step_counts[1], backward, lat_count, lon_count)
    back = march(g0 + back, step_counts[0], backward, lat_count, lon_count)
    return jnp.transpose(back.reshape(groups, rows * width, LANES), (0, 2, 1)).reshape(state.shape)


def solution(mesh):
    return jax.shard_map(
        partial(per_device, mesh.shape["lat"], mesh.shape["lon"]),
        mesh=mesh,
        in_specs=(
            P(None, None, "lat", "lon"),
            P(None, None, "lat", "lon"),
            P("lat", "lon"),
            P(None, ("lon", "lat")),
            P(None, ("lon", "lat"), None),
            P(),
            P(),
            P(),
            P(),
            P(),
            P(None, ("lon", "lat"), None, None, None),
        ),
        out_specs=P(None, None, "lat", "lon"),
        check_vma=False,
    )
```

```python
from functools import partial

import jax
import jax.numpy as jnp
from jax import lax
from jax.experimental import pallas as pl
from jax.experimental.pallas import tpu as pltpu
from jax.sharding import PartitionSpec as P

MAXSTEP = 4
LANES = 128
PAD = 8
MESH_ID = pl.DeviceIdType.MESH


def march_kernel(steps, lat_count, lon_count, x_ref, c_ref, o_ref, X, HL, ST, send_sem, recv_sem):
    groups, rows, width, _ = x_ref.shape
    lat = lax.axis_index("lat")
    lon = lax.axis_index("lon")
    east = lax.rem(lon + 1, lon_count)
    west = lax.rem(lon + lon_count - 1, lon_count)
    has_up = lat > 0
    has_down = lat < lat_count - 1
    inner = pl.ds(PAD, width)

    barrier = pltpu.get_barrier_semaphore()

    def greet(lat_to, lon_to):
        pl.semaphore_signal(barrier, inc=1, device_id={"lon": lon_to, "lat": lat_to}, device_id_type=MESH_ID)

    greet(lat, east)
    greet(lat, west)

    @pl.when(has_up)
    def _():
        greet(lat - 1, lon)

    @pl.when(has_down)
    def _():
        greet(lat + 1, lon)

    def to_up(p, g):
        return pltpu.make_async_remote_copy(
            X.at[p, g, 1, inner], X.at[p, g, rows + 1, inner],
            send_sem.at[p, g, 0], recv_sem.at[p, g, 0],
            device_id={"lon": lon, "lat": lat - 1}, device_id_type=MESH_ID)

    def to_down(p, g):
        return pltpu.make_async_remote_copy(
            X.at[p, g, rows, inner], X.at[p, g, 0, inner],
            send_sem.at[p, g, 1], recv_sem.at[p, g, 1],
            device_id={"lon": lon, "lat": lat + 1}, device_id_type=MESH_ID)

    def to_east(p, g):
        return pltpu.make_async_remote_copy(
            ST.at[p, g, 0], HL.at[p, g, 0],
            send_sem.at[p, g, 2], recv_sem.at[p, g, 2],
            device_id={"lon": east, "lat": lat}, device_id_type=MESH_ID)

    def to_west(p, g):
        return pltpu.make_async_remote_copy(
            ST.at[p, g, 1], HL.at[p, g, 1],
            send_sem.at[p, g, 3], recv_sem.at[p, g, 3],
            device_id={"lon": west, "lat": lat}, device_id_type=MESH_ID)

    def send(p, g):
        for r in range(rows):
            ST[p, g, 0, pl.ds(r, 1), :] = X[p, g, r + 1, pl.ds(PAD + width - 1, 1), :]
            ST[p, g, 1, pl.ds(r, 1), :] = X[p, g, r + 1, pl.ds(PAD, 1), :]

        @pl.when(has_up)
        def _():
            to_up(p, g).start()

        @pl.when(has_down)
        def _():
            to_down(p, g).start()

        to_east(p, g).start()
        to_west(p, g).start()

    def wait_send(p, g):
        @pl.when(has_up)
        def _():
            to_up(p, g).wait_send()

        @pl.when(has_down)
        def _():
            to_down(p, g).wait_send()

        to_east(p, g).wait_send()
        to_west(p, g).wait_send()

    def wait_recv(p, g):
        @pl.when(has_down)
        def _():
            to_up(p, g).wait_recv()

        @pl.when(has_up)
        def _():
            to_down(p, g).wait_recv()

        to_east(p, g).wait_recv()
        to_west(p, g).wait_recv()

    edge = jnp.zeros((width, LANES), jnp.float32)

    @pl.loop(0, groups)
    def _(g):
        for r in range(rows):
            X[0, g, r + 1, inner, :] = x_ref[g, r]
        for p in range(2):
            ST[p, g] = jnp.zeros(ST.shape[2:], jnp.float32)

            @pl.when(jnp.logical_not(has_up))
            def _():
                X[p, g, 0, inner, :] = edge

            @pl.when(jnp.logical_not(has_down))
            def _():
                X[p, g, rows + 1, inner, :] = edge

    pl.semaphore_wait(barrier, 2 + has_up.astype(jnp.int32) + has_down.astype(jnp.int32))

    @pl.loop(0, groups)
    def _(g):
        send(0, g)

    @pl.loop(0, steps * groups)
    def _(it):
        s = it // groups
        g = it % groups
        p = s % 2
        q = 1 - p
        wait_recv(p, g)

        @pl.when(s > 0)
        def _():
            wait_send(q, g)

        for r in range(rows):
            X[p, g, r + 1, pl.ds(PAD - 1, 1), :] = HL[p, g, 0, pl.ds(r, 1), :]
            X[p, g, r + 1, pl.ds(PAD + width, 1), :] = HL[p, g, 1, pl.ds(r, 1), :]
        for r in range(rows):
            for b in range(0, width, 64):
                at = pl.ds(PAD + b, 64)
                cat = pl.ds(b, 64)
                new = c_ref[0, r, cat, :] * X[p, g, r + 1, at, :]
                new = new + c_ref[3, r, cat, :] * X[p, g, r + 2, at, :]
                new = new + c_ref[4, r, cat, :] * X[p, g, r, at, :]
                new = new + c_ref[1, r, cat, :] * X[p, g, r + 1, pl.ds(PAD + b + 1, 64), :]
                new = new + c_ref[2, r, cat, :] * X[p, g, r + 1, pl.ds(PAD + b - 1, 64), :]
                X[q, g, r + 1, at, :] = new

        @pl.when(s < steps - 1)
        def _():
            send(q, g)

    @pl.loop(0, groups)
    def _(g):
        wait_send((steps - 1) % 2, g)
        for r in range(rows):
            o_ref[g, r] = X[steps % 2, g, r + 1, inner, :]


def march_call(steps, lat_count, lon_count, values, coef):
    groups, rows, width, lanes = values.shape
    edge_rows = -(-rows // 8) * 8
    vmem = pl.BlockSpec(memory_space=pltpu.VMEM)
    return pl.pallas_call(
        partial(march_kernel, steps, lat_count, lon_count),
        out_shape=jax.ShapeDtypeStruct(values.shape, jnp.float32),
        in_specs=[vmem, vmem],
        out_specs=vmem,
        scratch_shapes=[
            pltpu.VMEM((2, groups, rows + 2, width + 2 * PAD, lanes), jnp.float32),
            pltpu.VMEM((2, groups, 2, edge_rows, lanes), jnp.float32),
            pltpu.VMEM((2, groups, 2, edge_rows, lanes), jnp.float32),
            pltpu.SemaphoreType.DMA((2, groups, 4)),
            pltpu.SemaphoreType.DMA((2, groups, 4)),
        ],
        compiler_params=pltpu.CompilerParams(
            collective_id=steps, has_side_effects=True, vmem_limit_bytes=16 << 20
        ),
        cost_estimate=pl.CostEstimate(
            flops=9 * steps * values.size, bytes_accessed=8 * values.size * steps, transcendentals=0
        ),
        name="march",
    )(values, coef)


def march(values, count, coef, lat_count, lon_count):
    branches = [partial(march_call, n, lat_count, lon_count) for n in range(1, MAXSTEP + 1)]
    return lax.switch(count - 1, branches, values, coef)


def prep_kernel(lat_count, lon_count, state_ref, winds_ref, diff_ref, x_ref, fwd_ref, bwd_ref, lon_out,
                lon_in, lat_out, lat_in, send_sem, recv_sem):
    groups, rows, width, lanes = x_ref.shape
    levels = winds_ref.shape[0] // (2 * rows)
    lat = lax.axis_index("lat")
    lon = lax.axis_index("lon")
    east = lax.rem(lon + 1, lon_count)
    west = lax.rem(lon + lon_count - 1, lon_count)
    has_up = lat > 0
    has_down = lat < lat_count - 1
    barrier = pltpu.get_barrier_semaphore()

    def greet(lat_to, lon_to):
        pl.semaphore_signal(barrier, inc=1, device_id={"lon": lon_to, "lat": lat_to}, device_id_type=MESH_ID)

    greet(lat, east)
    greet(lat, west)

    @pl.when(has_up)
    def _():
        greet(lat - 1, lon)

    @pl.when(has_down)
    def _():
        greet(lat + 1, lon)

    def to_east():
        return pltpu.make_async_remote_copy(
            lon_out, lon_in, send_sem.at[0], recv_sem.at[0],
            device_id={"lon": east, "lat": lat}, device_id_type=MESH_ID)

    def to_down():
        return pltpu.make_async_remote_copy(
            lat_out, lat_in, send_sem.at[1], recv_sem.at[1],
            device_id={"lon": lon, "lat": lat + 1}, device_id_type=MESH_ID)

    def pair(i, r):
        w = winds_ref[pl.ds(i * levels * rows + r, levels, stride=rows), :] * 0.5
        d = diff_ref[pl.ds(r, 1), :]
        plus = jnp.concatenate([w + d] * (lanes // levels), axis=0).T
        minus = jnp.concatenate([w - d] * (lanes // levels), axis=0).T
        return plus, minus

    lon_out[...] = jnp.zeros(lon_out.shape, jnp.float32)
    for r in range(rows):
        a, b = pair(0, r)
        al, bl = pair(1, r)
        fwd_ref[1, r] = -b
        bwd_ref[1, r] = a
        fwd_ref[3, r] = -bl
        bwd_ref[3, r] = al
        lon_out[0, pl.ds(r, 1), :] = a[width - 1:width, :]
        lon_out[1, pl.ds(r, 1), :] = b[width - 1:width, :]
        if r == rows - 1:
            lat_out[0] = al
            lat_out[1] = bl

    @pl.when(jnp.logical_not(has_up))
    def _():
        lat_in[...] = jnp.zeros(lat_in.shape, jnp.float32)

    pl.semaphore_wait(barrier, 2 + has_up.astype(jnp.int32) + has_down.astype(jnp.int32))
    to_east().start()

    @pl.when(has_down)
    def _():
        to_down().start()

    for g in range(groups):
        for r in range(rows):
            x_ref[g, r] = state_ref[pl.ds(g * lanes * rows + r, lanes, stride=rows), :].T

    to_east().wait_recv()

    @pl.when(has_up)
    def _():
        to_down().wait_recv()

    first = lax.broadcasted_iota(jnp.int32, (width, lanes), 0) == 0
    for r in range(rows):
        a, b = bwd_ref[1, r], -fwd_ref[1, r]
        al, bl = bwd_ref[3, r], -fwd_ref[3, r]
        aw = jnp.where(first, lon_in[0, pl.ds(r, 1), :], pltpu.roll(a, 1, 0))
        bw = jnp.where(first, lon_in[1, pl.ds(r, 1), :], pltpu.roll(b, 1, 0))
        if r == 0:
            au, bu = lat_in[0], lat_in[1]
        else:
            au, bu = bwd_ref[3, r - 1], -fwd_ref[3, r - 1]
        centre = 1.0 - a + bw - al + bu
        fwd_ref[0, r] = centre
        bwd_ref[0, r] = centre
        fwd_ref[2, r] = aw
        bwd_ref[2, r] = -bw
        fwd_ref[4, r] = au
        bwd_ref[4, r] = -bu

    to_east().wait_send()

    @pl.when(has_down)
    def _():
        to_down().wait_send()


def prepare(state, winds, diffusivity, lat_count, lon_count):
    variables, levels, rows, width = state.shape
    groups = variables * levels // LANES
    edge_rows = -(-rows // 8) * 8
    vmem = pl.BlockSpec(memory_space=pltpu.VMEM)
    coef = jax.ShapeDtypeStruct((5, rows, width, LANES), jnp.float32)
    return pl.pallas_call(
        partial(prep_kernel, lat_count, lon_count),
        out_shape=[jax.ShapeDtypeStruct((groups, rows, width, LANES), jnp.float32), coef, coef],
        in_specs=[vmem] * 3,
        out_specs=[vmem] * 3,
        scratch_shapes=[
            pltpu.VMEM((2, edge_rows, LANES), jnp.float32),
            pltpu.VMEM((2, edge_rows, LANES), jnp.float32),
            pltpu.VMEM((2, width, LANES), jnp.float32),
            pltpu.VMEM((2, width, LANES), jnp.float32),
            pltpu.SemaphoreType.DMA((2,)),
            pltpu.SemaphoreType.DMA((2,)),
        ],
        compiler_params=pltpu.CompilerParams(
            collective_id=MAXSTEP + 1, has_side_effects=True, vmem_limit_bytes=16 << 20
        ),
        cost_estimate=pl.CostEstimate(flops=1 << 22, bytes_accessed=8 << 20, transcendentals=0),
        name="prepare",
    )(state.reshape(-1, width), winds.reshape(-1, width), diffusivity)


def split2(v):
    high = v.astype(jnp.bfloat16)
    return high, (v - high.astype(jnp.float32)).astype(jnp.bfloat16)


def split3(v):
    high = v.astype(jnp.bfloat16)
    rest = v - high.astype(jnp.float32)
    mid = rest.astype(jnp.bfloat16)
    return high, mid, (rest - mid.astype(jnp.float32)).astype(jnp.bfloat16)


def dot(a, b, dims=((1,), (0,))):
    return lax.dot_general(a, b, (dims, ((), ())), preferred_element_type=jnp.float32)


def pick(chosen, v, dims=((1,), (0,))):
    high, mid, low = split3(v)
    return dot(chosen, high, dims) + dot(chosen, mid, dims) + dot(chosen, low, dims)


def product(a, b, dims=((1,), (0,))):
    m = a[0].shape[0]
    both = dot(jnp.concatenate(a, axis=0), b[0], dims)
    return both[:m] + both[m:] + dot(a[0], b[1], dims)


def one_hot(row, size):
    return (row == lax.broadcasted_iota(jnp.int32, (size, row.shape[1]), 0)).astype(
        jnp.float32).astype(jnp.bfloat16)


def obs_kernel(capacity, x0_ref, x1_ref, cell_ref, owner_ref, got_ref, chan_ref,
               absorb_ref, emit_ref, weight_ref, g0_ref, g1_ref):
    groups, rows, width, lanes = x0_ref.shape
    cells = rows * width
    soundings = cell_ref.shape[1]
    channels = weight_ref.shape[1]
    fields = (x0_ref, x1_ref)
    outs = (g0_ref, g1_ref)
    first = ((0,), (0,))
    last = ((1,), (1,))
    picker = one_hot(chan_ref[...], channels)
    count = dot(jnp.ones((8, picker.shape[1]), jnp.bfloat16), picker, last)[0:1]
    absorb = split2(absorb_ref[...])
    emit = split2(emit_ref[...])
    weight = weight_ref[...]
    earlier = lax.broadcasted_iota(jnp.int32, (soundings, soundings), 0) < lax.broadcasted_iota(
        jnp.int32, (soundings, soundings), 1)
    placed, wanted, profile = [], [], []
    for k in range(2):
        placed.append(one_hot(cell_ref[k:k + 1, :], cells))
        owner = owner_ref[k]
        spread = jnp.broadcast_to(owner.astype(jnp.float32), (soundings, soundings))
        same = jnp.logical_and(spread.T == spread, earlier)
        rank = jnp.sum(same.astype(jnp.float32), axis=0, keepdims=True).astype(jnp.int32)
        source = one_hot(owner * capacity + rank, got_ref.shape[1])
        wanted.append(pick(source, got_ref[k], first))
        profile.append(jnp.concatenate(
            [pick(placed[k], fields[k][g].reshape(cells, lanes), first) for g in range(groups)], axis=1))
    parts = split3(jnp.concatenate(wanted, axis=0))
    m = 2 * soundings
    stacked = dot(jnp.concatenate(parts, axis=0), picker, last)
    wanted = stacked[:m] + stacked[m:2 * m] + stacked[2 * m:]
    profile = split2(jnp.concatenate(profile, axis=0))
    optical = product(profile, absorb, last)
    bright = product(profile, emit, last)
    small = jnp.exp(-jnp.abs(optical))
    inv = 1.0 / (1.0 + small)
    passed = jnp.where(optical > 0, small, 1.0) * inv
    slope = jnp.where(optical > 0, 1.0, small) * inv
    y = passed * bright
    departure = weight * (count * y - wanted)
    d_bright = split2(departure * passed)
    d_optical = split2(-(departure * y) * slope)
    back = product(d_optical, absorb) + product(d_bright, emit)
    for k in range(2):
        part = back[k * soundings:(k + 1) * soundings]
        for g in range(groups):
            outs[k][g] = pick(placed[k], part[:, g * lanes:(g + 1) * lanes]).reshape(rows, width, lanes)


def observe(x0, x1, sounding_cell, owners, fetched, channel_list, absorb, emit, weight, capacity):
    vmem = pl.BlockSpec(memory_space=pltpu.VMEM)
    return pl.pallas_call(
        partial(obs_kernel, capacity),
        out_shape=[jax.ShapeDtypeStruct(x0.shape, jnp.float32)] * 2,
        in_specs=[vmem] * 9,
        out_specs=[vmem] * 2,
        compiler_params=pltpu.CompilerParams(vmem_limit_bytes=56 << 20),
        cost_estimate=pl.CostEstimate(flops=6 << 30, bytes_accessed=8 << 20, transcendentals=0),
        name="observe",
    )(x0, x1, sounding_cell, owners, fetched, channel_list[None, :], absorb.T, emit.T, weight[None, :])


def per_device(lat_count, lon_count, state, winds, diffusivity, sounding_cell, sounding_owner,
               step_counts, channel_list, absorb_table, emit_table, obs_weight, observed):
    slots, _, devices, capacity, used = observed.shape
    fetched = lax.all_to_all(observed[:, 0], ("lon", "lat"), split_axis=1, concat_axis=1, tiled=True)
    fetched = fetched.reshape(slots, devices * capacity, used)
    x, forward, backward = prepare(state, winds, diffusivity, lat_count, lon_count)
    x0 = march(x, step_counts[0], forward, lat_count, lon_count)
    x1 = march(x0, step_counts[1], forward, lat_count, lon_count)
    owners = jnp.transpose(sounding_owner, (0, 2, 1))
    g0, g1 = observe(x0, x1, sounding_cell, owners, fetched, channel_list,
                     absorb_table, emit_table, obs_weight, capacity)
    back = march(g1, step_counts[1], backward, lat_count, lon_count)
    back = march(g0 + back, step_counts[0], backward, lat_count, lon_count)
    groups, rows, width, lanes = back.shape
    return jnp.transpose(back.reshape(groups, rows * width, lanes), (0, 2, 1)).reshape(state.shape)


def solution(mesh):
    return jax.shard_map(
        partial(per_device, mesh.shape["lat"], mesh.shape["lon"]),
        mesh=mesh,
        in_specs=(
            P(None, None, "lat", "lon"),
            P(None, None, "lat", "lon"),
            P("lat", "lon"),
            P(None, ("lon", "lat")),
            P(None, ("lon", "lat"), None),
            P(),
            P(),
            P(),
            P(),
            P(),
            P(None, ("lon", "lat"), None, None, None),
        ),
        out_specs=P(None, None, "lat", "lon"),
        check_vma=False,
    )
```

```python
from functools import partial

import jax
import jax.numpy as jnp
from jax import lax
from jax.experimental import pallas as pl
from jax.experimental.pallas import tpu as pltpu
from jax.sharding import PartitionSpec as P

MAXSTEP = 4
LANES = 128
PAD = 8
MESH_ID = pl.DeviceIdType.MESH


def march_kernel(steps, lat_count, lon_count, share, *refs):
    if share:
        (x_ref, c_ref, obs_ref, o_ref, got_ref, X, HL, ST, send_sem, recv_sem,
         share_send, share_recv) = refs
    else:
        x_ref, c_ref, o_ref, X, HL, ST, send_sem, recv_sem = refs
    groups, rows, width, _ = x_ref.shape
    lat = lax.axis_index("lat")
    lon = lax.axis_index("lon")
    east = lax.rem(lon + 1, lon_count)
    west = lax.rem(lon + lon_count - 1, lon_count)
    has_up = lat > 0
    has_down = lat < lat_count - 1
    inner = pl.ds(PAD, width)

    barrier = pltpu.get_barrier_semaphore()

    def greet(lat_to, lon_to):
        pl.semaphore_signal(barrier, inc=1, device_id={"lon": lon_to, "lat": lat_to}, device_id_type=MESH_ID)

    devices = lat_count * lon_count
    me = lon * lat_count + lat
    if share:
        @pl.loop(1, devices)
        def _(j):
            other = (me + j) % devices
            greet(other % lat_count, other // lat_count)

        greeted = devices - 1
    else:
        greet(lat, east)
        greet(lat, west)

        @pl.when(has_up)
        def _():
            greet(lat - 1, lon)

        @pl.when(has_down)
        def _():
            greet(lat + 1, lon)

        greeted = 2 + has_up.astype(jnp.int32) + has_down.astype(jnp.int32)

    def hand_over(j):
        other = (me + j) % devices
        return pltpu.make_async_remote_copy(
            obs_ref.at[other], got_ref.at[me], share_send.at[j], share_recv.at[j],
            device_id={"lon": other // lat_count, "lat": other % lat_count}, device_id_type=MESH_ID)

    def to_up(p, g):
        return pltpu.make_async_remote_copy(
            X.at[p, g, 1, inner], X.at[p, g, rows + 1, inner],
            send_sem.at[p, g, 0], recv_sem.at[p, g, 0],
            device_id={"lon": lon, "lat": lat - 1}, device_id_type=MESH_ID)

    def to_down(p, g):
        return pltpu.make_async_remote_copy(
            X.at[p, g, rows, inner], X.at[p, g, 0, inner],
            send_sem.at[p, g, 1], recv_sem.at[p, g, 1],
            device_id={"lon": lon, "lat": lat + 1}, device_id_type=MESH_ID)

    def to_east(p, g):
        return pltpu.make_async_remote_copy(
            ST.at[p, g, 0], HL.at[p, g, 0],
            send_sem.at[p, g, 2], recv_sem.at[p, g, 2],
            device_id={"lon": east, "lat": lat}, device_id_type=MESH_ID)

    def to_west(p, g):
        return pltpu.make_async_remote_copy(
            ST.at[p, g, 1], HL.at[p, g, 1],
            send_sem.at[p, g, 3], recv_sem.at[p, g, 3],
            device_id={"lon": west, "lat": lat}, device_id_type=MESH_ID)

    def send(p, g):
        for r in range(rows):
            ST[p, g, 0, pl.ds(r, 1), :] = X[p, g, r + 1, pl.ds(PAD + width - 1, 1), :]
            ST[p, g, 1, pl.ds(r, 1), :] = X[p, g, r + 1, pl.ds(PAD, 1), :]

        @pl.when(has_up)
        def _():
            to_up(p, g).start()

        @pl.when(has_down)
        def _():
            to_down(p, g).start()

        to_east(p, g).start()
        to_west(p, g).start()

    def wait_send(p, g):
        @pl.when(has_up)
        def _():
            to_up(p, g).wait_send()

        @pl.when(has_down)
        def _():
            to_down(p, g).wait_send()

        to_east(p, g).wait_send()
        to_west(p, g).wait_send()

    def wait_recv(p, g):
        @pl.when(has_down)
        def _():
            to_up(p, g).wait_recv()

        @pl.when(has_up)
        def _():
            to_down(p, g).wait_recv()

        to_east(p, g).wait_recv()
        to_west(p, g).wait_recv()

    edge = jnp.zeros((width, LANES), jnp.float32)

    @pl.loop(0, groups)
    def _(g):
        for r in range(rows):
            X[0, g, r + 1, inner, :] = x_ref[g, r]
        for p in range(2):
            ST[p, g] = jnp.zeros(ST.shape[2:], jnp.float32)

            @pl.when(jnp.logical_not(has_up))
            def _():
                X[p, g, 0, inner, :] = edge

            @pl.when(jnp.logical_not(has_down))
            def _():
                X[p, g, rows + 1, inner, :] = edge

    pl.semaphore_wait(barrier, greeted)

    @pl.loop(0, groups)
    def _(g):
        send(0, g)

    turn = -(-(devices - 1) // (steps * groups))
    if share:
        got_ref[me] = obs_ref[me]

    @pl.loop(0, steps * groups)
    def _(it):
        s = it // groups
        g = it % groups
        if share:
            @pl.loop(0, turn)
            def _(i):
                j = 1 + it * turn + i

                @pl.when(j < devices)
                def _():
                    hand_over(j).start()

        p = s % 2
        q = 1 - p
        wait_recv(p, g)

        @pl.when(s > 0)
        def _():
            wait_send(q, g)

        for r in range(rows):
            X[p, g, r + 1, pl.ds(PAD - 1, 1), :] = HL[p, g, 0, pl.ds(r, 1), :]
            X[p, g, r + 1, pl.ds(PAD + width, 1), :] = HL[p, g, 1, pl.ds(r, 1), :]
        for r in range(rows):
            for b in range(0, width, 64):
                at = pl.ds(PAD + b, 64)
                cat = pl.ds(b, 64)
                new = c_ref[0, r, cat, :] * X[p, g, r + 1, at, :]
                new = new + c_ref[3, r, cat, :] * X[p, g, r + 2, at, :]
                new = new + c_ref[4, r, cat, :] * X[p, g, r, at, :]
                new = new + c_ref[1, r, cat, :] * X[p, g, r + 1, pl.ds(PAD + b + 1, 64), :]
                new = new + c_ref[2, r, cat, :] * X[p, g, r + 1, pl.ds(PAD + b - 1, 64), :]
                X[q, g, r + 1, at, :] = new

        @pl.when(s < steps - 1)
        def _():
            send(q, g)

    @pl.loop(0, groups)
    def _(g):
        wait_send((steps - 1) % 2, g)
        for r in range(rows):
            o_ref[g, r] = X[steps % 2, g, r + 1, inner, :]

    if share:
        @pl.loop(1, devices)
        def _(j):
            hand_over(j).wait_send()
            hand_over(j).wait_recv()


def march_call(steps, lat_count, lon_count, values, coef, *obs):
    groups, rows, width, lanes = values.shape
    edge_rows = -(-rows // 8) * 8
    share = len(obs)
    devices = lat_count * lon_count
    vmem = pl.BlockSpec(memory_space=pltpu.VMEM)
    scratch = [
        pltpu.VMEM((2, groups, rows + 2, width + 2 * PAD, lanes), jnp.float32),
        pltpu.VMEM((2, groups, 2, edge_rows, lanes), jnp.float32),
        pltpu.VMEM((2, groups, 2, edge_rows, lanes), jnp.float32),
        pltpu.SemaphoreType.DMA((2, groups, 4)),
        pltpu.SemaphoreType.DMA((2, groups, 4)),
    ] + [pltpu.SemaphoreType.DMA((devices,))] * (2 * share)
    out = [jax.ShapeDtypeStruct(v.shape, jnp.float32) for v in (values, *obs)]
    return pl.pallas_call(
        partial(march_kernel, steps, lat_count, lon_count, share),
        out_shape=out,
        in_specs=[vmem] * (2 + share),
        out_specs=[vmem] * (1 + share),
        scratch_shapes=scratch,
        compiler_params=pltpu.CompilerParams(
            collective_id=steps + (MAXSTEP + 1) * (1 - share), has_side_effects=True,
            vmem_limit_bytes=20 << 20
        ),
        cost_estimate=pl.CostEstimate(
            flops=9 * steps * values.size, bytes_accessed=8 * values.size * steps, transcendentals=0
        ),
        name="share" if share else "march",
    )(values, coef, *obs)


def march(values, count, coef, lat_count, lon_count, *obs):
    branches = [partial(march_call, n, lat_count, lon_count) for n in range(1, MAXSTEP + 1)]
    return lax.switch(count - 1, branches, values, coef, *obs)


def prep_kernel(lat_count, lon_count, state_ref, winds_ref, diff_ref, obs_ref, x_ref, fwd_ref, bwd_ref, obs0_ref, obs1_ref, lon_out,
                lon_in, lat_out, lat_in, send_sem, recv_sem):
    groups, rows, width, lanes = x_ref.shape
    levels = winds_ref.shape[0] // (2 * rows)
    lat = lax.axis_index("lat")
    lon = lax.axis_index("lon")
    east = lax.rem(lon + 1, lon_count)
    west = lax.rem(lon + lon_count - 1, lon_count)
    has_up = lat > 0
    has_down = lat < lat_count - 1
    barrier = pltpu.get_barrier_semaphore()

    def greet(lat_to, lon_to):
        pl.semaphore_signal(barrier, inc=1, device_id={"lon": lon_to, "lat": lat_to}, device_id_type=MESH_ID)

    greet(lat, east)
    greet(lat, west)

    @pl.when(has_up)
    def _():
        greet(lat - 1, lon)

    @pl.when(has_down)
    def _():
        greet(lat + 1, lon)

    def to_east():
        return pltpu.make_async_remote_copy(
            lon_out, lon_in, send_sem.at[0], recv_sem.at[0],
            device_id={"lon": east, "lat": lat}, device_id_type=MESH_ID)

    def to_down():
        return pltpu.make_async_remote_copy(
            lat_out, lat_in, send_sem.at[1], recv_sem.at[1],
            device_id={"lon": lon, "lat": lat + 1}, device_id_type=MESH_ID)

    def pair(i, r):
        w = winds_ref[pl.ds(i * levels * rows + r, levels, stride=rows), :] * 0.5
        d = diff_ref[pl.ds(r, 1), :]
        plus = jnp.concatenate([w + d] * (lanes // levels), axis=0).T
        minus = jnp.concatenate([w - d] * (lanes // levels), axis=0).T
        return plus, minus

    lon_out[...] = jnp.zeros(lon_out.shape, jnp.float32)
    for r in range(rows):
        a, b = pair(0, r)
        al, bl = pair(1, r)
        fwd_ref[1, r] = -b
        bwd_ref[1, r] = a
        fwd_ref[3, r] = -bl
        bwd_ref[3, r] = al
        lon_out[0, pl.ds(r, 1), :] = a[width - 1:width, :]
        lon_out[1, pl.ds(r, 1), :] = b[width - 1:width, :]
        if r == rows - 1:
            lat_out[0] = al
            lat_out[1] = bl

    @pl.when(jnp.logical_not(has_up))
    def _():
        lat_in[...] = jnp.zeros(lat_in.shape, jnp.float32)

    pl.semaphore_wait(barrier, 2 + has_up.astype(jnp.int32) + has_down.astype(jnp.int32))
    to_east().start()

    @pl.when(has_down)
    def _():
        to_down().start()

    for g in range(groups):
        for r in range(rows):
            x_ref[g, r] = state_ref[pl.ds(g * lanes * rows + r, lanes, stride=rows), :].T

    slots, capacity, devices, used = obs_ref.shape
    chunks = used // lanes
    stride = obs0_ref.shape[0] // devices
    for k, out in enumerate((obs0_ref, obs1_ref)):
        for c in range(capacity):
            for h in range(chunks):
                out[pl.ds(c * chunks + h, devices, stride=stride), :] = obs_ref[k, c, :, pl.ds(h * lanes, lanes)]
        for c in range(capacity * chunks, stride):
            out[pl.ds(c, devices, stride=stride), :] = jnp.zeros((devices, lanes), jnp.float32)

    to_east().wait_recv()

    @pl.when(has_up)
    def _():
        to_down().wait_recv()

    first = lax.broadcasted_iota(jnp.int32, (width, lanes), 0) == 0
    for r in range(rows):
        a, b = bwd_ref[1, r], -fwd_ref[1, r]
        al, bl = bwd_ref[3, r], -fwd_ref[3, r]
        aw = jnp.where(first, lon_in[0, pl.ds(r, 1), :], pltpu.roll(a, 1, 0))
        bw = jnp.where(first, lon_in[1, pl.ds(r, 1), :], pltpu.roll(b, 1, 0))
        if r == 0:
            au, bu = lat_in[0], lat_in[1]
        else:
            au, bu = bwd_ref[3, r - 1], -fwd_ref[3, r - 1]
        centre = 1.0 - a + bw - al + bu
        fwd_ref[0, r] = centre
        bwd_ref[0, r] = centre
        fwd_ref[2, r] = aw
        bwd_ref[2, r] = -bw
        fwd_ref[4, r] = au
        bwd_ref[4, r] = -bu

    to_east().wait_send()

    @pl.when(has_down)
    def _():
        to_down().wait_send()


def prepare(state, winds, diffusivity, observed, lat_count, lon_count):
    slots, _, devices, capacity, used = observed.shape
    block = -(-capacity * (used // LANES) // 8) * 8
    handed = jax.ShapeDtypeStruct((devices * block, LANES), jnp.float32)
    by_rank = jnp.transpose(observed[:, 0], (0, 2, 1, 3))
    variables, levels, rows, width = state.shape
    groups = variables * levels // LANES
    edge_rows = -(-rows // 8) * 8
    vmem = pl.BlockSpec(memory_space=pltpu.VMEM)
    coef = jax.ShapeDtypeStruct((5, rows, width, LANES), jnp.float32)
    return pl.pallas_call(
        partial(prep_kernel, lat_count, lon_count),
        out_shape=[jax.ShapeDtypeStruct((groups, rows, width, LANES), jnp.float32), coef, coef, handed, handed],
        in_specs=[vmem] * 4,
        out_specs=[vmem] * 5,
        scratch_shapes=[
            pltpu.VMEM((2, edge_rows, LANES), jnp.float32),
            pltpu.VMEM((2, edge_rows, LANES), jnp.float32),
            pltpu.VMEM((2, width, LANES), jnp.float32),
            pltpu.VMEM((2, width, LANES), jnp.float32),
            pltpu.SemaphoreType.DMA((2,)),
            pltpu.SemaphoreType.DMA((2,)),
        ],
        compiler_params=pltpu.CompilerParams(
            collective_id=2 * MAXSTEP + 2, has_side_effects=True, vmem_limit_bytes=16 << 20
        ),
        cost_estimate=pl.CostEstimate(flops=1 << 22, bytes_accessed=8 << 20, transcendentals=0),
        name="prepare",
    )(state.reshape(-1, width), winds.reshape(-1, width), diffusivity, by_rank)


def split2(v):
    high = v.astype(jnp.bfloat16)
    return high, (v - high.astype(jnp.float32)).astype(jnp.bfloat16)


def split3(v):
    high = v.astype(jnp.bfloat16)
    rest = v - high.astype(jnp.float32)
    mid = rest.astype(jnp.bfloat16)
    return high, mid, (rest - mid.astype(jnp.float32)).astype(jnp.bfloat16)


def dot(a, b, dims=((1,), (0,))):
    return lax.dot_general(a, b, (dims, ((), ())), preferred_element_type=jnp.float32)


def pick(chosen, v, dims=((1,), (0,))):
    high, mid, low = split3(v)
    return dot(chosen, high, dims) + dot(chosen, mid, dims) + dot(chosen, low, dims)


def product(a, b, dims=((1,), (0,))):
    m = a[0].shape[0]
    both = dot(jnp.concatenate(a, axis=0), b[0], dims)
    return both[:m] + both[m:] + dot(a[0], b[1], dims)


def one_hot(row, size):
    return (row == lax.broadcasted_iota(jnp.int32, (size, row.shape[1]), 0)).astype(
        jnp.float32).astype(jnp.bfloat16)


def obs_kernel(x0_ref, x1_ref, cell_ref, owner_ref, got0_ref, got1_ref, chan_ref,
               absorb_ref, emit_ref, weight_ref, g0_ref, g1_ref):
    groups, rows, width, lanes = x0_ref.shape
    cells = rows * width
    soundings = cell_ref.shape[1]
    channels = weight_ref.shape[1]
    fields = (x0_ref, x1_ref)
    outs = (g0_ref, g1_ref)
    gots = (got0_ref, got1_ref)
    chunks = chan_ref.shape[1] // lanes
    devices, block, _ = got0_ref.shape
    capacity = block // chunks
    first = ((0,), (0,))
    last = ((1,), (1,))
    picker = one_hot(chan_ref[...], channels)
    count = dot(jnp.ones((8, picker.shape[1]), jnp.bfloat16), picker, last)[0:1]
    absorb = split2(absorb_ref[...])
    emit = split2(emit_ref[...])
    weight = weight_ref[...]
    earlier = lax.broadcasted_iota(jnp.int32, (soundings, soundings), 0) < lax.broadcasted_iota(
        jnp.int32, (soundings, soundings), 1)
    placed, wanted, profile = [], [], []
    for k in range(2):
        placed.append(one_hot(cell_ref[k:k + 1, :], cells))
        owner = owner_ref[k]
        spread = jnp.broadcast_to(owner.astype(jnp.float32), (soundings, soundings))
        same = jnp.logical_and(spread.T == spread, earlier)
        rank = jnp.sum(same.astype(jnp.float32), axis=0, keepdims=True).astype(jnp.int32)
        source = one_hot(owner * capacity + rank, devices * capacity)
        got = gots[k].reshape(devices * block, lanes)
        wanted.append(jnp.concatenate(
            [pick(source, got[pl.ds(h, devices * capacity, stride=chunks), :], first) for h in range(chunks)], axis=1))
        profile.append(jnp.concatenate(
            [pick(placed[k], fields[k][g].reshape(cells, lanes), first) for g in range(groups)], axis=1))
    parts = split3(jnp.concatenate(wanted, axis=0))
    m = 2 * soundings
    stacked = dot(jnp.concatenate(parts, axis=0), picker, last)
    wanted = stacked[:m] + stacked[m:2 * m] + stacked[2 * m:]
    profile = split2(jnp.concatenate(profile, axis=0))
    optical = product(profile, absorb, last)
    bright = product(profile, emit, last)
    small = jnp.exp(-jnp.abs(optical))
    inv = 1.0 / (1.0 + small)
    passed = jnp.where(optical > 0, small, 1.0) * inv
    slope = jnp.where(optical > 0, 1.0, small) * inv
    y = passed * bright
    departure = weight * (count * y - wanted)
    d_bright = split2(departure * passed)
    d_optical = split2(-(departure * y) * slope)
    back = product(d_optical, absorb) + product(d_bright, emit)
    for k in range(2):
        part = back[k * soundings:(k + 1) * soundings]
        for g in range(groups):
            outs[k][g] = pick(placed[k], part[:, g * lanes:(g + 1) * lanes]).reshape(rows, width, lanes)


def observe(x0, x1, sounding_cell, owners, got0, got1, channel_list, absorb, emit, weight):
    vmem = pl.BlockSpec(memory_space=pltpu.VMEM)
    return pl.pallas_call(
        obs_kernel,
        out_shape=[jax.ShapeDtypeStruct(x0.shape, jnp.float32)] * 2,
        in_specs=[vmem] * 10,
        out_specs=[vmem] * 2,
        compiler_params=pltpu.CompilerParams(vmem_limit_bytes=56 << 20),
        cost_estimate=pl.CostEstimate(flops=6 << 30, bytes_accessed=8 << 20, transcendentals=0),
        name="observe",
    )(x0, x1, sounding_cell, owners, got0, got1, channel_list[None, :], absorb.T, emit.T, weight[None, :])


def per_device(lat_count, lon_count, state, winds, diffusivity, sounding_cell, sounding_owner,
               step_counts, channel_list, absorb_table, emit_table, obs_weight, observed):
    devices = observed.shape[2]
    x, forward, backward, obs0, obs1 = prepare(state, winds, diffusivity, observed, lat_count, lon_count)
    obs0 = obs0.reshape(devices, -1, LANES)
    obs1 = obs1.reshape(devices, -1, LANES)
    x0, got0 = march(x, step_counts[0], forward, lat_count, lon_count, obs0)
    x1, got1 = march(x0, step_counts[1], forward, lat_count, lon_count, obs1)
    owners = jnp.transpose(sounding_owner, (0, 2, 1))
    g0, g1 = observe(x0, x1, sounding_cell, owners, got0, got1, channel_list,
                     absorb_table, emit_table, obs_weight)
    (back,) = march(g1, step_counts[1], backward, lat_count, lon_count)
    (back,) = march(g0 + back, step_counts[0], backward, lat_count, lon_count)
    groups, rows, width, lanes = back.shape
    return jnp.transpose(back.reshape(groups, rows * width, lanes), (0, 2, 1)).reshape(state.shape)


def solution(mesh):
    return jax.shard_map(
        partial(per_device, mesh.shape["lat"], mesh.shape["lon"]),
        mesh=mesh,
        in_specs=(
            P(None, None, "lat", "lon"),
            P(None, None, "lat", "lon"),
            P("lat", "lon"),
            P(None, ("lon", "lat")),
            P(None, ("lon", "lat"), None),
            P(),
            P(),
            P(),
            P(),
            P(),
            P(None, ("lon", "lat"), None, None, None),
        ),
        out_specs=P(None, None, "lat", "lon"),
        check_vma=False,
    )
```

```python
from functools import partial

import jax
import jax.numpy as jnp
from jax import lax
from jax.experimental import pallas as pl
from jax.experimental.pallas import tpu as pltpu
from jax.sharding import PartitionSpec as P

MAXSTEP = 4
LANES = 128
PAD = 8
MESH_ID = pl.DeviceIdType.MESH


def march_kernel(steps, lat_count, lon_count, share, last, *refs):
    if share:
        (x_ref, c_ref, obs_ref, o_ref, got_ref, X, HL, ST, send_sem, recv_sem,
         share_send, share_recv) = refs
    elif last:
        x_ref, c_ref, g_ref, o_ref, X, HL, ST, send_sem, recv_sem = refs
    else:
        x_ref, c_ref, o_ref, X, HL, ST, send_sem, recv_sem = refs
    groups, rows, width, _ = x_ref.shape
    lat = lax.axis_index("lat")
    lon = lax.axis_index("lon")
    east = lax.rem(lon + 1, lon_count)
    west = lax.rem(lon + lon_count - 1, lon_count)
    has_up = lat > 0
    has_down = lat < lat_count - 1
    inner = pl.ds(PAD, width)

    barrier = pltpu.get_barrier_semaphore()

    def greet(lat_to, lon_to):
        pl.semaphore_signal(barrier, inc=1, device_id={"lon": lon_to, "lat": lat_to}, device_id_type=MESH_ID)

    devices = lat_count * lon_count
    me = lon * lat_count + lat
    if share:
        @pl.loop(1, devices)
        def _(j):
            other = (me + j) % devices
            greet(other % lat_count, other // lat_count)

        greeted = devices - 1
    else:
        greet(lat, east)
        greet(lat, west)

        @pl.when(has_up)
        def _():
            greet(lat - 1, lon)

        @pl.when(has_down)
        def _():
            greet(lat + 1, lon)

        greeted = 2 + has_up.astype(jnp.int32) + has_down.astype(jnp.int32)

    def hand_over(j):
        other = (me + j) % devices
        return pltpu.make_async_remote_copy(
            obs_ref.at[other], got_ref.at[me], share_send.at[j], share_recv.at[j],
            device_id={"lon": other // lat_count, "lat": other % lat_count}, device_id_type=MESH_ID)

    def to_up(p, g):
        return pltpu.make_async_remote_copy(
            X.at[p, g, 1, inner], X.at[p, g, rows + 1, inner],
            send_sem.at[p, g, 0], recv_sem.at[p, g, 0],
            device_id={"lon": lon, "lat": lat - 1}, device_id_type=MESH_ID)

    def to_down(p, g):
        return pltpu.make_async_remote_copy(
            X.at[p, g, rows, inner], X.at[p, g, 0, inner],
            send_sem.at[p, g, 1], recv_sem.at[p, g, 1],
            device_id={"lon": lon, "lat": lat + 1}, device_id_type=MESH_ID)

    def to_east(p, g):
        return pltpu.make_async_remote_copy(
            ST.at[p, g, 0], HL.at[p, g, 0],
            send_sem.at[p, g, 2], recv_sem.at[p, g, 2],
            device_id={"lon": east, "lat": lat}, device_id_type=MESH_ID)

    def to_west(p, g):
        return pltpu.make_async_remote_copy(
            ST.at[p, g, 1], HL.at[p, g, 1],
            send_sem.at[p, g, 3], recv_sem.at[p, g, 3],
            device_id={"lon": west, "lat": lat}, device_id_type=MESH_ID)

    def send(p, g):
        for r in range(rows):
            ST[p, g, 0, pl.ds(r, 1), :] = X[p, g, r + 1, pl.ds(PAD + width - 1, 1), :]
            ST[p, g, 1, pl.ds(r, 1), :] = X[p, g, r + 1, pl.ds(PAD, 1), :]

        @pl.when(has_up)
        def _():
            to_up(p, g).start()

        @pl.when(has_down)
        def _():
            to_down(p, g).start()

        to_east(p, g).start()
        to_west(p, g).start()

    def wait_send(p, g):
        @pl.when(has_up)
        def _():
            to_up(p, g).wait_send()

        @pl.when(has_down)
        def _():
            to_down(p, g).wait_send()

        to_east(p, g).wait_send()
        to_west(p, g).wait_send()

    def wait_recv(p, g):
        @pl.when(has_down)
        def _():
            to_up(p, g).wait_recv()

        @pl.when(has_up)
        def _():
            to_down(p, g).wait_recv()

        to_east(p, g).wait_recv()
        to_west(p, g).wait_recv()

    edge = jnp.zeros((width, LANES), jnp.float32)

    @pl.loop(0, groups)
    def _(g):
        for r in range(rows):
            X[0, g, r + 1, inner, :] = x_ref[g, r] + g_ref[g, r] if last else x_ref[g, r]
        for p in range(2):
            ST[p, g] = jnp.zeros(ST.shape[2:], jnp.float32)

            @pl.when(jnp.logical_not(has_up))
            def _():
                X[p, g, 0, inner, :] = edge

            @pl.when(jnp.logical_not(has_down))
            def _():
                X[p, g, rows + 1, inner, :] = edge

    pl.semaphore_wait(barrier, greeted)

    @pl.loop(0, groups)
    def _(g):
        send(0, g)

    turn = -(-(devices - 1) // (steps * groups))
    if share:
        got_ref[me] = obs_ref[me]

    @pl.loop(0, steps * groups)
    def _(it):
        s = it // groups
        g = it % groups
        if share:
            @pl.loop(0, turn)
            def _(i):
                j = 1 + it * turn + i

                @pl.when(j < devices)
                def _():
                    hand_over(j).start()

        p = s % 2
        q = 1 - p
        wait_recv(p, g)

        @pl.when(s > 0)
        def _():
            wait_send(q, g)

        for r in range(rows):
            X[p, g, r + 1, pl.ds(PAD - 1, 1), :] = HL[p, g, 0, pl.ds(r, 1), :]
            X[p, g, r + 1, pl.ds(PAD + width, 1), :] = HL[p, g, 1, pl.ds(r, 1), :]
        for r in range(rows):
            for b in range(0, width, 64):
                at = pl.ds(PAD + b, 64)
                cat = pl.ds(b, 64)
                new = c_ref[0, r, cat, :] * X[p, g, r + 1, at, :]
                new = new + c_ref[3, r, cat, :] * X[p, g, r + 2, at, :]
                new = new + c_ref[4, r, cat, :] * X[p, g, r, at, :]
                new = new + c_ref[1, r, cat, :] * X[p, g, r + 1, pl.ds(PAD + b + 1, 64), :]
                new = new + c_ref[2, r, cat, :] * X[p, g, r + 1, pl.ds(PAD + b - 1, 64), :]
                X[q, g, r + 1, at, :] = new

        @pl.when(s < steps - 1)
        def _():
            send(q, g)

    @pl.loop(0, groups)
    def _(g):
        wait_send((steps - 1) % 2, g)
        for r in range(rows):
            o_ref[g, r] = X[steps % 2, g, r + 1, inner, :]

    if share:
        @pl.loop(1, devices)
        def _(j):
            hand_over(j).wait_send()
            hand_over(j).wait_recv()


def march_call(steps, lat_count, lon_count, last, values, coef, *obs):
    groups, rows, width, lanes = values.shape
    edge_rows = -(-rows // 8) * 8
    share = len(obs) * (1 - last)
    devices = lat_count * lon_count
    vmem = pl.BlockSpec(memory_space=pltpu.VMEM)
    scratch = [
        pltpu.VMEM((2, groups, rows + 2, width + 2 * PAD, lanes), jnp.float32),
        pltpu.VMEM((2, groups, 2, edge_rows, lanes), jnp.float32),
        pltpu.VMEM((2, groups, 2, edge_rows, lanes), jnp.float32),
        pltpu.SemaphoreType.DMA((2, groups, 4)),
        pltpu.SemaphoreType.DMA((2, groups, 4)),
    ] + [pltpu.SemaphoreType.DMA((devices,))] * (2 * share)
    out = [jax.ShapeDtypeStruct(v.shape, jnp.float32) for v in (values, *obs)[:1 + share]]
    return pl.pallas_call(
        partial(march_kernel, steps, lat_count, lon_count, share, last),
        out_shape=out,
        in_specs=[vmem] * (2 + len(obs)),
        out_specs=[vmem] * (1 + share),
        scratch_shapes=scratch,
        compiler_params=pltpu.CompilerParams(
            collective_id=steps + (MAXSTEP + 1) * (1 - share) + (MAXSTEP + 2) * last, has_side_effects=True,
            vmem_limit_bytes=20 << 20
        ),
        cost_estimate=pl.CostEstimate(
            flops=9 * steps * values.size, bytes_accessed=8 * values.size * steps, transcendentals=0
        ),
        name="share" if share else "march",
    )(values, coef, *obs)


def march(values, count, coef, lat_count, lon_count, *obs, last=0):
    branches = [partial(march_call, n, lat_count, lon_count, last) for n in range(1, MAXSTEP + 1)]
    return lax.switch(count - 1, branches, values, coef, *obs)


def prep_kernel(lat_count, lon_count, state_ref, winds_ref, diff_ref, obs_ref, x_ref, fwd_ref, bwd_ref, obs0_ref, obs1_ref, lon_out,
                lon_in, lat_out, lat_in, send_sem, recv_sem):
    groups, rows, width, lanes = x_ref.shape
    levels = winds_ref.shape[0] // (2 * rows)
    lat = lax.axis_index("lat")
    lon = lax.axis_index("lon")
    east = lax.rem(lon + 1, lon_count)
    west = lax.rem(lon + lon_count - 1, lon_count)
    has_up = lat > 0
    has_down = lat < lat_count - 1
    barrier = pltpu.get_barrier_semaphore()

    def greet(lat_to, lon_to):
        pl.semaphore_signal(barrier, inc=1, device_id={"lon": lon_to, "lat": lat_to}, device_id_type=MESH_ID)

    greet(lat, east)
    greet(lat, west)

    @pl.when(has_up)
    def _():
        greet(lat - 1, lon)

    @pl.when(has_down)
    def _():
        greet(lat + 1, lon)

    def to_east():
        return pltpu.make_async_remote_copy(
            lon_out, lon_in, send_sem.at[0], recv_sem.at[0],
            device_id={"lon": east, "lat": lat}, device_id_type=MESH_ID)

    def to_down():
        return pltpu.make_async_remote_copy(
            lat_out, lat_in, send_sem.at[1], recv_sem.at[1],
            device_id={"lon": lon, "lat": lat + 1}, device_id_type=MESH_ID)

    def pair(i, r):
        w = winds_ref[pl.ds(i * levels * rows + r, levels, stride=rows), :] * 0.5
        d = diff_ref[pl.ds(r, 1), :]
        plus = jnp.concatenate([w + d] * (lanes // levels), axis=0).T
        minus = jnp.concatenate([w - d] * (lanes // levels), axis=0).T
        return plus, minus

    lon_out[...] = jnp.zeros(lon_out.shape, jnp.float32)
    for r in range(rows):
        a, b = pair(0, r)
        al, bl = pair(1, r)
        fwd_ref[1, r] = -b
        bwd_ref[1, r] = a
        fwd_ref[3, r] = -bl
        bwd_ref[3, r] = al
        lon_out[0, pl.ds(r, 1), :] = a[width - 1:width, :]
        lon_out[1, pl.ds(r, 1), :] = b[width - 1:width, :]
        if r == rows - 1:
            lat_out[0] = al
            lat_out[1] = bl

    @pl.when(jnp.logical_not(has_up))
    def _():
        lat_in[...] = jnp.zeros(lat_in.shape, jnp.float32)

    pl.semaphore_wait(barrier, 2 + has_up.astype(jnp.int32) + has_down.astype(jnp.int32))
    to_east().start()

    @pl.when(has_down)
    def _():
        to_down().start()

    for g in range(groups):
        for r in range(rows):
            x_ref[g, r] = state_ref[pl.ds(g * lanes * rows + r, lanes, stride=rows), :].T

    slots, capacity, devices, used = obs_ref.shape
    chunks = used // lanes
    stride = obs0_ref.shape[0] // devices
    for k, out in enumerate((obs0_ref, obs1_ref)):
        for c in range(capacity):
            for h in range(chunks):
                out[pl.ds(c * chunks + h, devices, stride=stride), :] = obs_ref[k, c, :, pl.ds(h * lanes, lanes)]
        for c in range(capacity * chunks, stride):
            out[pl.ds(c, devices, stride=stride), :] = jnp.zeros((devices, lanes), jnp.float32)

    to_east().wait_recv()

    @pl.when(has_up)
    def _():
        to_down().wait_recv()

    first = lax.broadcasted_iota(jnp.int32, (width, lanes), 0) == 0
    for r in range(rows):
        a, b = bwd_ref[1, r], -fwd_ref[1, r]
        al, bl = bwd_ref[3, r], -fwd_ref[3, r]
        aw = jnp.where(first, lon_in[0, pl.ds(r, 1), :], pltpu.roll(a, 1, 0))
        bw = jnp.where(first, lon_in[1, pl.ds(r, 1), :], pltpu.roll(b, 1, 0))
        if r == 0:
            au, bu = lat_in[0], lat_in[1]
        else:
            au, bu = bwd_ref[3, r - 1], -fwd_ref[3, r - 1]
        centre = 1.0 - a + bw - al + bu
        fwd_ref[0, r] = centre
        bwd_ref[0, r] = centre
        fwd_ref[2, r] = aw
        bwd_ref[2, r] = -bw
        fwd_ref[4, r] = au
        bwd_ref[4, r] = -bu

    to_east().wait_send()

    @pl.when(has_down)
    def _():
        to_down().wait_send()


def prepare(state, winds, diffusivity, observed, lat_count, lon_count):
    slots, _, devices, capacity, used = observed.shape
    block = -(-capacity * (used // LANES) // 8) * 8
    handed = jax.ShapeDtypeStruct((devices * block, LANES), jnp.float32)
    by_rank = jnp.transpose(observed[:, 0], (0, 2, 1, 3))
    variables, levels, rows, width = state.shape
    groups = variables * levels // LANES
    edge_rows = -(-rows // 8) * 8
    vmem = pl.BlockSpec(memory_space=pltpu.VMEM)
    coef = jax.ShapeDtypeStruct((5, rows, width, LANES), jnp.float32)
    return pl.pallas_call(
        partial(prep_kernel, lat_count, lon_count),
        out_shape=[jax.ShapeDtypeStruct((groups, rows, width, LANES), jnp.float32), coef, coef, handed, handed],
        in_specs=[vmem] * 4,
        out_specs=[vmem] * 5,
        scratch_shapes=[
            pltpu.VMEM((2, edge_rows, LANES), jnp.float32),
            pltpu.VMEM((2, edge_rows, LANES), jnp.float32),
            pltpu.VMEM((2, width, LANES), jnp.float32),
            pltpu.VMEM((2, width, LANES), jnp.float32),
            pltpu.SemaphoreType.DMA((2,)),
            pltpu.SemaphoreType.DMA((2,)),
        ],
        compiler_params=pltpu.CompilerParams(
            collective_id=2 * MAXSTEP + 2, has_side_effects=True, vmem_limit_bytes=16 << 20
        ),
        cost_estimate=pl.CostEstimate(flops=1 << 22, bytes_accessed=8 << 20, transcendentals=0),
        name="prepare",
    )(state.reshape(-1, width), winds.reshape(-1, width), diffusivity, by_rank)


def split2(v):
    high = v.astype(jnp.bfloat16)
    return high, (v - high.astype(jnp.float32)).astype(jnp.bfloat16)


def split3(v):
    high = v.astype(jnp.bfloat16)
    rest = v - high.astype(jnp.float32)
    mid = rest.astype(jnp.bfloat16)
    return high, mid, (rest - mid.astype(jnp.float32)).astype(jnp.bfloat16)


def dot(a, b, dims=((1,), (0,))):
    return lax.dot_general(a, b, (dims, ((), ())), preferred_element_type=jnp.float32)


def pick(chosen, v, dims=((1,), (0,))):
    high, mid, low = split3(v)
    return dot(chosen, high, dims) + dot(chosen, mid, dims) + dot(chosen, low, dims)


def product(a, b, dims=((1,), (0,))):
    m = a[0].shape[0]
    both = dot(jnp.concatenate(a, axis=0), b[0], dims)
    return both[:m] + both[m:] + dot(a[0], b[1], dims)


def one_hot(row, size):
    return (row == lax.broadcasted_iota(jnp.int32, (size, row.shape[1]), 0)).astype(
        jnp.float32).astype(jnp.bfloat16)


def obs_kernel(x0_ref, x1_ref, cell_ref, owner_ref, got0_ref, got1_ref, chan_ref,
               absorb_ref, emit_ref, weight_ref, g0_ref, g1_ref):
    groups, rows, width, lanes = x0_ref.shape
    cells = rows * width
    soundings = cell_ref.shape[1]
    channels = weight_ref.shape[1]
    fields = (x0_ref, x1_ref)
    outs = (g0_ref, g1_ref)
    gots = (got0_ref, got1_ref)
    chunks = chan_ref.shape[1] // lanes
    devices, block, _ = got0_ref.shape
    capacity = block // chunks
    first = ((0,), (0,))
    last = ((1,), (1,))
    picker = one_hot(chan_ref[...], channels)
    count = dot(jnp.ones((8, picker.shape[1]), jnp.bfloat16), picker, last)[0:1]
    absorb = split2(absorb_ref[...])
    emit = split2(emit_ref[...])
    weight = weight_ref[...]
    earlier = lax.broadcasted_iota(jnp.int32, (soundings, soundings), 0) < lax.broadcasted_iota(
        jnp.int32, (soundings, soundings), 1)
    placed, wanted, profile = [], [], []
    for k in range(2):
        placed.append(one_hot(cell_ref[k:k + 1, :], cells))
        owner = owner_ref[k]
        spread = jnp.broadcast_to(owner.astype(jnp.float32), (soundings, soundings))
        same = jnp.logical_and(spread.T == spread, earlier)
        rank = jnp.sum(same.astype(jnp.float32), axis=0, keepdims=True).astype(jnp.int32)
        source = one_hot(owner * capacity + rank, devices * capacity)
        got = gots[k].reshape(devices * block, lanes)
        wanted.append(jnp.concatenate(
            [pick(source, got[pl.ds(h, devices * capacity, stride=chunks), :], first) for h in range(chunks)], axis=1))
        profile.append(jnp.concatenate(
            [pick(placed[k], fields[k][g].reshape(cells, lanes), first) for g in range(groups)], axis=1))
    parts = split3(jnp.concatenate(wanted, axis=0))
    m = 2 * soundings
    stacked = dot(jnp.concatenate(parts, axis=0), picker, last)
    wanted = stacked[:m] + stacked[m:2 * m] + stacked[2 * m:]
    profile = split2(jnp.concatenate(profile, axis=0))
    optical = product(profile, absorb, last)
    bright = product(profile, emit, last)
    small = jnp.exp(-jnp.abs(optical))
    inv = 1.0 / (1.0 + small)
    passed = jnp.where(optical > 0, small, 1.0) * inv
    slope = jnp.where(optical > 0, 1.0, small) * inv
    y = passed * bright
    departure = weight * (count * y - wanted)
    d_bright = split2(departure * passed)
    d_optical = split2(-(departure * y) * slope)
    back = product(d_optical, absorb) + product(d_bright, emit)
    for k in range(2):
        part = back[k * soundings:(k + 1) * soundings]
        for g in range(groups):
            outs[k][g] = pick(placed[k], part[:, g * lanes:(g + 1) * lanes]).reshape(rows, width, lanes)


def observe(x0, x1, sounding_cell, owners, got0, got1, channel_list, absorb, emit, weight):
    vmem = pl.BlockSpec(memory_space=pltpu.VMEM)
    return pl.pallas_call(
        obs_kernel,
        out_shape=[jax.ShapeDtypeStruct(x0.shape, jnp.float32)] * 2,
        in_specs=[vmem] * 10,
        out_specs=[vmem] * 2,
        compiler_params=pltpu.CompilerParams(vmem_limit_bytes=56 << 20),
        cost_estimate=pl.CostEstimate(flops=6 << 30, bytes_accessed=8 << 20, transcendentals=0),
        name="observe",
    )(x0, x1, sounding_cell, owners, got0, got1, channel_list[None, :], absorb.T, emit.T, weight[None, :])


def per_device(lat_count, lon_count, state, winds, diffusivity, sounding_cell, sounding_owner,
               step_counts, channel_list, absorb_table, emit_table, obs_weight, observed):
    devices = observed.shape[2]
    x, forward, backward, obs0, obs1 = prepare(state, winds, diffusivity, observed, lat_count, lon_count)
    obs0 = obs0.reshape(devices, -1, LANES)
    obs1 = obs1.reshape(devices, -1, LANES)
    x0, got0 = march(x, step_counts[0], forward, lat_count, lon_count, obs0)
    x1, got1 = march(x0, step_counts[1], forward, lat_count, lon_count, obs1)
    owners = jnp.transpose(sounding_owner, (0, 2, 1))
    g0, g1 = observe(x0, x1, sounding_cell, owners, got0, got1, channel_list,
                     absorb_table, emit_table, obs_weight)
    (back,) = march(g1, step_counts[1], backward, lat_count, lon_count)
    (back,) = march(back, step_counts[0], backward, lat_count, lon_count, g0, last=1)
    groups, rows, width, lanes = back.shape
    return jnp.transpose(back.reshape(groups, rows * width, lanes), (0, 2, 1)).reshape(state.shape)


def solution(mesh):
    return jax.shard_map(
        partial(per_device, mesh.shape["lat"], mesh.shape["lon"]),
        mesh=mesh,
        in_specs=(
            P(None, None, "lat", "lon"),
            P(None, None, "lat", "lon"),
            P("lat", "lon"),
            P(None, ("lon", "lat")),
            P(None, ("lon", "lat"), None),
            P(),
            P(),
            P(),
            P(),
            P(),
            P(None, ("lon", "lat"), None, None, None),
        ),
        out_specs=P(None, None, "lat", "lon"),
        check_vma=False,
    )
```
